16 devices in a mesh: dp: 4 (over z, y), tp: 4 (over x, core).
Axes of the slice: x: 2, y: 2, z: 2, core: 2. Of those that a mesh axis runs over, the one named last changes fastest.
Arguments:
- hidden_in: bfloat16 [4, 256, 6144], P('dp'), parts along dimension 0
- lengths: int32 [4], P('dp'), parts along dimension 0
- positions: int32 [4, 256], P('dp'), parts along dimension 0
- ln_gain: float32 [2, 2, 6144], replicated
- ln_bias: float32 [2, 2, 6144], replicated
- w_query: bfloat16 [2, 6144, 48, 128], P(None, None, 'tp')
- w_key: bfloat16 [2, 6144, 8, 128], replicated
- w_value: bfloat16 [2, 6144, 8, 128], replicated
- w_out: bfloat16 [2, 48, 128, 6144], P(None, 'tp')
- w_up: bfloat16 [2, 6144, 24576], P(None, None, 'tp')
- w_down: bfloat16 [2, 24576, 6144], P(None, 'tp')
Outputs:
- output 1: bfloat16 [4, 256, 6144], P('dp'), parts along dimension 0
- output 2: bfloat16 [2, 4, 256, 8, 128], P(None, 'dp', None, 'tp'), parts along dimension 1
- output 3: bfloat16 [2, 4, 256, 8, 128], P(None, 'dp', None, 'tp'), parts along dimension 1
There are 4 independent parts. The reference program is written for one: setup_inputs(seed, part) draws one part's arguments, and reference() takes and returns one part's arrays. A program takes and returns all parts, laid end to end along the dimension named above; an argument that names none is the same for every part.
All inputs are finite; a program needn't handle non-finite values.
Results may differ from the reference program's by a relative error of at most 0.02.
Values are sent between devices in bfloat16 or wider.
A program may use at most 1.75 GiB of HBM per device.

```python
import jax
import jax.numpy as jnp
from jax import lax

D = 6144
HEADS = 48
KV_HEADS = 8
HEAD = 128
FF = 24576
BATCH = 1
SEQ = 256
LAYERS = 2
KV_SLOTS = 8
GROUP = HEADS // KV_HEADS
ROT = HEAD // 2
SCALE = HEAD ** -0.5
ROPE_BASE = 10000.0
NORM_EPS = 1e-5


def setup_inputs(seed: int = 0, part: int = 0) -> dict:
    base_key = jax.random.key(seed)
    shared_keys = jax.random.split(base_key, 8)
    part_keys = jax.random.split(jax.random.fold_in(base_key, part), 3)
    hidden_in = jax.random.normal(part_keys[0], (BATCH, SEQ, D), jnp.float32).astype(jnp.bfloat16)
    lengths = jax.random.randint(part_keys[1], (BATCH,), max(1, SEQ // 4), SEQ + 1).astype(jnp.int32)
    offsets = jax.random.randint(part_keys[2], (BATCH, 1), 0, 4096)
    positions = (offsets + jnp.arange(SEQ)[None, :]).astype(jnp.int32)
    ln_gain = 0.3 * jax.random.normal(shared_keys[0], (LAYERS, 2, D), jnp.float32)
    ln_bias = 0.3 * jax.random.normal(shared_keys[1], (LAYERS, 2, D), jnp.float32)
    w_query = (jax.random.normal(shared_keys[2], (LAYERS, D, HEADS, HEAD), jnp.float32) * (1.2 * D ** -0.5)).astype(jnp.bfloat16)
    w_key = (jax.random.normal(shared_keys[3], (LAYERS, D, KV_HEADS, HEAD), jnp.float32) * (1.2 * D ** -0.5)).astype(jnp.bfloat16)
    w_value = (jax.random.normal(shared_keys[4], (LAYERS, D, KV_HEADS, HEAD), jnp.float32) * D ** -0.5).astype(jnp.bfloat16)
    w_out = (jax.random.normal(shared_keys[5], (LAYERS, HEADS, HEAD, D), jnp.float32) * (2.0 * (HEADS * HEAD) ** -0.5)).astype(jnp.bfloat16)
    w_up = (jax.random.normal(shared_keys[6], (LAYERS, D, FF), jnp.float32) * D ** -0.5).astype(jnp.bfloat16)
    w_down = (jax.random.normal(shared_keys[7], (LAYERS, FF, D), jnp.float32) * FF ** -0.5).astype(jnp.bfloat16)
    return {"hidden_in": hidden_in, "lengths": lengths, "positions": positions, "ln_gain": ln_gain, "ln_bias": ln_bias, "w_query": w_query, "w_key": w_key, "w_value": w_value, "w_out": w_out, "w_up": w_up, "w_down": w_down}


def layer_norm(hidden, gain, bias):
    values = hidden.astype(jnp.float32)
    average = jnp.mean(values, axis=-1, keepdims=True)
    centred = values - average
    variance = jnp.mean(centred * centred, axis=-1, keepdims=True)
    normed = centred * lax.rsqrt(variance + NORM_EPS) * (1.0 + gain) + bias
    return normed.astype(jnp.bfloat16)


def rotary_embed(values, positions):
    half_width = ROT // 2
    frequencies = ROPE_BASE ** (-2.0 * jnp.arange(half_width, dtype=jnp.float32) / ROT)
    angles = positions.astype(jnp.float32)[..., None] * frequencies
    cosine = jnp.cos(angles)[..., None, :]
    sine = jnp.sin(angles)[..., None, :]
    first = values[..., :half_width]
    second = values[..., half_width:ROT]
    return jnp.concatenate([first * cosine - second * sine, second * cosine + first * sine, values[..., ROT:]], axis=-1)


def attend_row(row_args):
    query, key_row, value_row, length = row_args
    query = query.reshape(SEQ, KV_HEADS, GROUP, HEAD).astype(jnp.float32)
    scores = jnp.einsum("qkgd,skd->kgqs", query, key_row.astype(jnp.float32)) * SCALE
    query_pos = jnp.arange(SEQ)[:, None]
    key_pos = jnp.arange(SEQ)[None, :]
    allowed = (key_pos <= query_pos) & (key_pos < length)
    attn_weights = jax.nn.softmax(jnp.where(allowed, scores, -1e30), axis=-1)
    mixed = jnp.einsum("kgqs,skd->qkgd", attn_weights, value_row.astype(jnp.float32))
    return mixed.reshape(SEQ, HEADS * HEAD).astype(jnp.bfloat16)


def reference(hidden_in, lengths, positions, ln_gain, ln_bias, w_query, w_key, w_value, w_out, w_up, w_down):
    tokens = BATCH * SEQ
    valid = (jnp.arange(SEQ)[None, :] < lengths[:, None])[:, :, None, None]

    def layer_step(hidden, weights):
        gain, bias, q_weight, k_weight, v_weight, o_weight, up_weight, down_weight = weights
        normed = layer_norm(hidden, gain[0], bias[0]).reshape(tokens, D)
        query_lin = jnp.dot(normed, q_weight.reshape(D, HEADS * HEAD), preferred_element_type=jnp.float32)
        key_lin = jnp.dot(normed, k_weight.reshape(D, KV_HEADS * HEAD), preferred_element_type=jnp.float32)
        value_lin = jnp.dot(normed, v_weight.reshape(D, KV_HEADS * HEAD), preferred_element_type=jnp.float32)
        query = rotary_embed(query_lin.reshape(BATCH, SEQ, HEADS, HEAD), positions).astype(jnp.bfloat16)
        keys = rotary_embed(key_lin.reshape(BATCH, SEQ, KV_HEADS, HEAD), positions).astype(jnp.bfloat16)
        values = value_lin.reshape(BATCH, SEQ, KV_HEADS, HEAD).astype(jnp.bfloat16)
        mixed = lax.map(attend_row, (query, keys, values, lengths))
        attn_out = jnp.dot(mixed.reshape(tokens, HEADS * HEAD), o_weight.reshape(HEADS * HEAD, D), preferred_element_type=jnp.float32).astype(jnp.bfloat16)
        residual = (hidden.astype(jnp.float32) + attn_out.reshape(BATCH, SEQ, D).astype(jnp.float32)).astype(jnp.bfloat16)
        normed_mlp = layer_norm(residual, gain[1], bias[1]).reshape(tokens, D)
        up_lin = jnp.dot(normed_mlp, up_weight, preferred_element_type=jnp.float32)
        activated = jnp.maximum(up_lin, 0.0)
        activated = (activated * activated).astype(jnp.bfloat16)
        mlp_out = jnp.dot(activated, down_weight, preferred_element_type=jnp.float32).astype(jnp.bfloat16)
        new_hidden = (residual.astype(jnp.float32) + mlp_out.reshape(BATCH, SEQ, D).astype(jnp.float32)).astype(jnp.bfloat16)
        key_store = jnp.where(valid, jnp.repeat(keys, KV_SLOTS // KV_HEADS, axis=2), 0.0).astype(jnp.bfloat16)
        value_store = jnp.where(valid, jnp.repeat(values, KV_SLOTS // KV_HEADS, axis=2), 0.0).astype(jnp.bfloat16)
        return new_hidden, (key_store, value_store)

    hidden_out, caches = lax.scan(layer_step, hidden_in, (ln_gain, ln_bias, w_query, w_key, w_value, w_out, w_up, w_down))
    return hidden_out, caches[0], caches[1]
```

```python
import functools

import jax
import jax.numpy as jnp
from jax import lax
from jax.experimental import pallas as pl
from jax.experimental.pallas import tpu as pltpu
from jax.sharding import PartitionSpec as P

ROPE_BASE = 10000.0
NORM_EPS = 1e-5
CH = 512
RING = 6
KV_RING = 4
MESH = pl.DeviceIdType.MESH
F32 = jnp.float32
BF16 = jnp.bfloat16


def kernel(cfg, hid, tabs, mask, valid, gain, bias, wq, wk, wv, wo, wu, wd,
           out, kc, vc,
           wbuf, kraw, vraw, wkv, hbuf, acc, abuf, pbuf, rbuf, xrecv, xres,
           wsem, ksem, vsem, iosem,
           d_send, d_recv, x_send, x_recv,
           gx_send, gx_recv, gc_send, gc_recv, gf_send, gf_recv):
    layers, seq, d, heads, scale = cfg
    nch = d // CH
    qw = heads * 128
    nq = qw // CH
    quarter = seq // 4
    half = seq // 2
    kper = nch // nq

    me = lax.axis_index("tp")
    mx = me // 2
    mc = me % 2
    core_peer = {"tp": mx * 2 + (1 - mc)}
    chip_peer = {"tp": (1 - mx) * 2 + mc}
    own_rows = pl.ds(pl.multiple_of(half * mc + quarter * mx, quarter), quarter)
    peer_rows = pl.ds(pl.multiple_of(half * mc + quarter * (1 - mx), quarter), quarter)
    away_rows = pl.ds(pl.multiple_of(half * (1 - mc), half), half)
    own_part = pl.ds(pl.multiple_of(quarter * mx, quarter), quarter)
    peer_part = pl.ds(pl.multiple_of(quarter * (1 - mx), quarter), quarter)

    def cols(j):
        if isinstance(j, int):
            return pl.ds(j * CH, CH)
        return pl.ds(pl.multiple_of(j * CH, CH), CH)

    def fetch_q(l, i, slot):
        rows = kper * CH
        for n in range(nq):
            for hh in range(4):
                pltpu.make_async_copy(
                    wq.at[l, 4 * n + hh, pl.ds(pl.multiple_of(i * rows, rows), rows), :],
                    wbuf.at[slot, pl.ds(n * rows, rows), pl.ds(hh * 128, 128)],
                    wsem.at[slot]).start()

    def fetch_o(l, i, slot):
        for n in range(kper):
            pltpu.make_async_copy(
                wo.at[l, :, cols(i * kper + n)],
                wbuf.at[slot, pl.ds(n * qw, qw), :],
                wsem.at[slot]).start()

    def fetch_u(l, i, slot):
        for n in range(nch):
            pltpu.make_async_copy(
                wu.at[l, cols(i), pl.ds(n * CH, CH)],
                wbuf.at[slot, pl.ds(n * CH, CH), :],
                wsem.at[slot]).start()

    def fetch_d(l, i, slot):
        pltpu.make_async_copy(wd.at[l, :, cols(i)], wbuf.at[slot], wsem.at[slot]).start()

    def weights_ready(slot):
        pltpu.make_async_copy(wd.at[0, :, pl.ds(0, CH)], wbuf.at[slot], wsem.at[slot]).wait()

    def kv_copies(l, kk):
        slot = kk % KV_RING
        rows = cols(kk)
        return (pltpu.make_async_copy(wk.at[l, rows, me], kraw.at[slot], ksem.at[slot]),
                pltpu.make_async_copy(wv.at[l, rows, me], vraw.at[slot], vsem.at[slot]))

    def kv_fetch(l, kk):
        for c in kv_copies(l, kk):
            c.start()

    def remote(src, dst, ssem, rsem, peer):
        return pltpu.make_async_remote_copy(
            src_ref=src, dst_ref=dst, send_sem=ssem, recv_sem=rsem,
            device_id=peer, device_id_type=MESH)

    def d_copy(j):
        return remote(pbuf.at[away_rows, cols(j)], rbuf.at[:, cols(j)],
                      d_send.at[j], d_recv.at[j], core_peer)

    def x_copy(j):
        return remote(pbuf.at[peer_rows, cols(j)], xrecv.at[:, cols(j)],
                      x_send.at[j], x_recv.at[j], chip_peer)

    def rs_mid(j):
        d_copy(j).wait_recv()
        s = pbuf[peer_rows, cols(j)].astype(F32) + rbuf[peer_part, cols(j)].astype(F32)
        pbuf[peer_rows, cols(j)] = s.astype(BF16)
        x_copy(j).start()

    def rs_fin(j):
        x_copy(j).wait_recv()
        s = pbuf[own_rows, cols(j)].astype(F32) + rbuf[own_part, cols(j)].astype(F32)
        s = (s + xrecv[:, cols(j)].astype(F32)).astype(BF16)
        new = (xres[:, cols(j)].astype(F32) + s.astype(F32)).astype(BF16)
        xres[:, cols(j)] = new
        return new

    def gx_copy(j):
        r = hbuf.at[own_rows, cols(j)]
        return remote(r, r, gx_send.at[j], gx_recv.at[j], chip_peer)

    def gc_copy(j):
        r = hbuf.at[own_rows, cols(j)]
        return remote(r, r, gc_send.at[j], gc_recv.at[j], core_peer)

    def gf_copy(j):
        r = hbuf.at[peer_rows, cols(j)]
        return remote(r, r, gf_send.at[j], gf_recv.at[j], core_peer)

    def forward(j):
        gx_copy(j).wait_recv()
        gf_copy(j).start()

    def gathered(j):
        gc_copy(j).wait_recv()
        gf_copy(j).wait_recv()

    def loop(n, body):
        lax.fori_loop(0, n, lambda i, c: (body(i), c)[1], 0)

    def gather_sent():
        def body(j):
            gx_copy(j).wait_send()
            gc_copy(j).wait_send()
            gf_copy(j).wait_send()
        loop(nch, body)

    def norm_rows(src, src_rows, dst_rows, row, after):
        zero = jnp.zeros((quarter, CH), F32)
        total = lax.fori_loop(
            0, nch, lambda j, t: t + src[src_rows, cols(j)].astype(F32), zero)
        mean = jnp.sum(total, axis=-1, keepdims=True) * (1.0 / d)

        def squares(j, t):
            x = src[src_rows, cols(j)].astype(F32) - mean
            return t + x * x

        var = jnp.sum(lax.fori_loop(0, nch, squares, zero), axis=-1, keepdims=True) * (1.0 / d)
        rstd = lax.rsqrt(var + NORM_EPS)

        def write(j):
            x = (src[src_rows, cols(j)].astype(F32) - mean) * rstd
            y = x * (1.0 + gain[pl.ds(row, 1), cols(j)]) + bias[pl.ds(row, 1), cols(j)]
            hbuf[dst_rows, cols(j)] = y.astype(BF16)
            after(j)

        loop(nch, write)

    def norm_and_send(row):
        def after(j):
            gx_copy(j).start()
            gc_copy(j).start()
        norm_rows(xres, pl.ds(0, quarter), own_rows, row, after)

    def clear(width):
        def body(i):
            acc[pl.ds(pl.multiple_of(i * 16, 16), 16), pl.ds(0, width)] = jnp.zeros((16, width), F32)
        loop(seq // 16, body)

    def project(l):
        clear(qw + CH)
        if l > 0:
            forward(0)

        def group(i):
            slot = i
            weights_ready(slot)

            def chunk(kq):
                kk = i * kper + kq
                if l > 0:
                    @pl.when(kk + 1 < nch)
                    def _():
                        forward(kk + 1)
                    gathered(kk)
                for c in kv_copies(l, kk):
                    c.wait()
                ks = kk % KV_RING
                for n in range(2):
                    wkv[:, pl.ds(n * 128, 128)] = kraw[ks, :, n, :]
                    wkv[:, pl.ds((n + 2) * 128, 128)] = vraw[ks, :, n, :]
                hk = hbuf[:, cols(kk)]
                for n in range(nq):
                    w = wbuf[slot, pl.ds(pl.multiple_of(n * kper * CH + kq * CH, CH), CH), :]
                    acc[:, pl.ds(n * CH, CH)] += jnp.dot(hk, w, preferred_element_type=F32)
                acc[:, pl.ds(qw, CH)] += jnp.dot(hk, wkv[...], preferred_element_type=F32)
                if KV_RING:
                    @pl.when(kk + KV_RING < nch)
                    def _():
                        kv_fetch(l, kk + KV_RING)
                    if l + 1 < layers:
                        @pl.when(kk + KV_RING >= nch)
                        def _():
                            kv_fetch(l + 1, kk + KV_RING - nch)

            loop(kper, chunk)
            fetch_u(l, i, slot)

        loop(nq, group)
        if l > 0:
            gather_sent()

    def attention(l):
        cosine, sin_a, sin_b = tabs[0], tabs[1], tabs[2]
        live = valid[...]

        def rope(x):
            return (x * cosine + pltpu.roll(x, 96, 1) * sin_a + pltpu.roll(x, 32, 1) * sin_b).astype(BF16)

        for n in range(2):
            k = rope(acc[:, pl.ds(qw + n * 128, 128)])
            v = acc[:, pl.ds(qw + (n + 2) * 128, 128)].astype(BF16)
            abuf[:, pl.ds(qw + n * 128, 128)] = k
            abuf[:, pl.ds(qw + (n + 2) * 128, 128)] = v
            kc[l, n] = (k.astype(F32) * live).astype(BF16)
            vc[l, n] = (v.astype(F32) * live).astype(BF16)

        group = heads // 2

        def body(i):
            for n in range(2):
                lanes = pl.ds(pl.multiple_of((n * group + i) * 128, 128), 128)
                q = rope(acc[:, lanes])
                k = abuf[:, pl.ds(qw + n * 128, 128)]
                v = abuf[:, pl.ds(qw + (n + 2) * 128, 128)]
                s = lax.dot_general(q, k, (((1,), (1,)), ((), ())), preferred_element_type=F32) * scale
                s = jnp.where(mask[...] > 0.5, s, -1e30)
                e = jnp.exp(s - jnp.max(s, axis=-1, keepdims=True))
                p = (e / jnp.sum(e, axis=-1, keepdims=True)).astype(BF16)
                abuf[:, lanes] = jnp.dot(p, v, preferred_element_type=F32).astype(BF16)

        loop(group, body)

    def rs_drain():
        def body(j):
            d_copy(j).wait_send()
            x_copy(j).wait_send()
        loop(nch, body)

    def project_out(l):
        def group(i):
            slot = nq + i
            weights_ready(slot)

            def chunk(n):
                j = i * kper + n
                w = wbuf[slot, pl.ds(pl.multiple_of(n * qw, qw), qw), :]
                pbuf[:, cols(j)] = jnp.dot(abuf[:, pl.ds(0, qw)], w, preferred_element_type=F32).astype(BF16)
                d_copy(j).start()

                @pl.when(j >= 1)
                def _():
                    rs_mid(j - 1)

            loop(kper, chunk)
            fetch_u(l, nq + i, slot)

        loop(nq, group)
        rs_mid(nch - 1)
        loop(nch, lambda j: (rs_fin(j), None)[1])
        rs_drain()

    def mlp_up(l):
        clear(d)
        forward(0)

        def group(i):
            slot = i % RING

            @pl.when(i + 1 < nch)
            def _():
                forward(i + 1)
            gathered(i)
            weights_ready(slot)
            hk = hbuf[:, cols(i)]
            for n in range(nch):
                acc[:, pl.ds(n * CH, CH)] += jnp.dot(
                    hk, wbuf[slot, pl.ds(n * CH, CH), :], preferred_element_type=F32)

            @pl.when(i < nch - RING)
            def _():
                fetch_u(l, i + RING, slot)

            @pl.when(i >= nch - RING)
            def _():
                fetch_d(l, i + RING - nch, slot)

        loop(nch, group)
        gather_sent()

        def square(j):
            u = jnp.maximum(acc[:, cols(j)], 0.0)
            abuf[:, cols(j)] = (u * u).astype(BF16)

        loop(nch, square)

    def finish(j):
        hbuf[own_rows, cols(j)] = rs_fin(j)
        gx_copy(j).start()
        gc_copy(j).start()

    def mlp_down(l):
        last = l + 1 == layers

        def group(j):
            slot = j % RING
            weights_ready(slot)
            pbuf[:, cols(j)] = jnp.dot(abuf[...], wbuf[slot], preferred_element_type=F32).astype(BF16)
            d_copy(j).start()

            @pl.when(j < nch - RING)
            def _():
                fetch_d(l, j + RING, slot)
            if not last:
                @pl.when((j >= nch - RING) & (j < nch - RING + nq))
                def _():
                    fetch_q(l + 1, j - (nch - RING), slot)

                @pl.when(j >= nch - RING + nq)
                def _():
                    fetch_o(l + 1, j - (nch - RING + nq), slot)

            @pl.when(j >= 1)
            def _():
                rs_mid(j - 1)
            if last:
                @pl.when(j >= 3)
                def _():
                    finish(j - 3)

                @pl.when(j >= 5)
                def _():
                    forward(j - 5)

        loop(nch, group)
        rs_mid(nch - 1)
        if not last:
            loop(nch, lambda j: (rs_fin(j), None)[1])
        else:
            for j in range(nch - 3, nch):
                finish(j)
            for j in range(nch - 5, nch):
                forward(j)
            loop(nch, gathered)
        rs_drain()

    load = pltpu.make_async_copy(hid.at[0], pbuf, iosem.at[0])
    load.start()
    for kk in range(KV_RING):
        kv_fetch(0, kk)
    for i in range(nq):
        fetch_q(0, i, i)
    for i in range(nq):
        fetch_o(0, i, nq + i)

    barrier = pltpu.get_barrier_semaphore()
    for peer in (core_peer, chip_peer):
        pl.semaphore_signal(barrier, inc=1, device_id=peer, device_id_type=MESH)
    pl.semaphore_wait(barrier, 2)

    load.wait()
    xres[...] = pbuf[own_rows, :]

    def first_norm(b):
        rows = pl.ds(pl.multiple_of(b * quarter, quarter), quarter)
        norm_rows(pbuf, rows, rows, 0, lambda j: None)

    loop(4, first_norm)

    for l in range(layers):
        project(l)
        attention(l)
        project_out(l)
        norm_and_send(2 * l + 1)
        mlp_up(l)
        mlp_down(l)
        if l + 1 < layers:
            norm_and_send(2 * l + 2)

    gather_sent()
    store = pltpu.make_async_copy(hbuf, out.at[0], iosem.at[1])
    store.start()
    store.wait()


def solution(mesh):
    def device_body(hidden_in, lengths, positions, ln_gain, ln_bias, w_query, w_key, w_value, w_out, w_up, w_down):
        seq, d = hidden_in.shape[1], hidden_in.shape[2]
        layers, _, heads, head = w_query.shape
        kv_heads = w_key.shape[2]
        tp = mesh.shape["tp"]
        kv = kv_heads // tp
        nch = d // CH

        half_rot = head // 4
        lane = jnp.arange(head)
        freq = ROPE_BASE ** (-2.0 * jnp.arange(half_rot, dtype=F32) / (2 * half_rot))
        angle = positions[0].astype(F32)[:, None] * freq
        cos, sin = jnp.cos(angle), jnp.sin(angle)
        zero, one = jnp.zeros((seq, half_rot), F32), jnp.ones((seq, 2 * half_rot), F32)
        zero2 = jnp.zeros((seq, 2 * half_rot), F32)
        tabs = jnp.stack([
            jnp.concatenate([cos, cos, one], -1),
            jnp.concatenate([-sin, zero, zero2], -1),
            jnp.concatenate([zero, sin, zero2], -1)])
        pos = jnp.arange(seq)
        mask = ((pos[None, :] <= pos[:, None]) & (pos[None, :] < lengths[0])).astype(F32)
        valid = jnp.broadcast_to((pos < lengths[0]).astype(F32)[:, None], (seq, head))

        vmem = pl.BlockSpec(memory_space=pltpu.VMEM)
        anym = pl.BlockSpec(memory_space=pl.ANY)
        dma = pltpu.SemaphoreType.DMA
        cfg = (layers, seq, d, heads, head ** -0.5)
        out, kc, vc = pl.pallas_call(
            functools.partial(kernel, cfg),
            out_shape=(jax.ShapeDtypeStruct((1, seq, d), BF16),
                       jax.ShapeDtypeStruct((layers, kv, seq, head), BF16),
                       jax.ShapeDtypeStruct((layers, kv, seq, head), BF16)),
            in_specs=[anym, vmem, vmem, vmem, vmem, vmem] + [anym] * 6,
            out_specs=(anym, vmem, vmem),
            scratch_shapes=[
                pltpu.VMEM((RING, d, CH), BF16),
                pltpu.VMEM((KV_RING, CH, kv, head), BF16),
                pltpu.VMEM((KV_RING, CH, kv, head), BF16),
                pltpu.VMEM((CH, CH), BF16),
                pltpu.VMEM((seq, d), BF16),
                pltpu.VMEM((seq, d), F32),
                pltpu.VMEM((seq, d), BF16),
                pltpu.VMEM((seq, d), BF16),
                pltpu.VMEM((seq // 2, d), BF16),
                pltpu.VMEM((seq // 4, d), BF16),
                pltpu.VMEM((seq // 4, d), BF16),
                dma((RING,)), dma((KV_RING,)), dma((KV_RING,)), dma((2,)),
            ] + [dma((nch,))] * 10,
            compiler_params=pltpu.CompilerParams(
                collective_id=0, has_side_effects=True, vmem_limit_bytes=67043328),
            name="decoder_layers",
        )(hidden_in, tabs, mask, valid,
          ln_gain.reshape(2 * layers, d), ln_bias.reshape(2 * layers, d),
          w_query.transpose(0, 2, 1, 3),
          w_key.reshape(layers, d, tp, kv, head), w_value.reshape(layers, d, tp, kv, head),
          w_out.reshape(layers, heads * head, d), w_up, w_down)
        kc = kc.transpose(0, 2, 1, 3)[:, None]
        vc = vc.transpose(0, 2, 1, 3)[:, None]
        return out, kc, vc

    specs_in = (P("dp", None, None), P("dp"), P("dp", None), P(), P(), P(None, None, "tp", None), P(), P(),
                P(None, "tp", None, None), P(None, None, "tp"), P(None, "tp", None))
    cache_spec = P(None, "dp", None, "tp", None)
    return jax.shard_map(device_body, mesh=mesh, in_specs=specs_in,
                         out_specs=(P("dp", None, None), cache_spec, cache_spec), check_vma=False)
```

```python
import functools

import jax
import jax.numpy as jnp
from jax import lax
from jax.experimental import pallas as pl
from jax.experimental.pallas import tpu as pltpu
from jax.sharding import PartitionSpec as P

ROPE_BASE = 10000.0
NORM_EPS = 1e-5
CH = 512
RING = 6
KV_RING = 2
LAG = 2
EARLY = 2
VMEM_LIMIT = 63360000
MESH = pl.DeviceIdType.MESH
F32 = jnp.float32
BF16 = jnp.bfloat16


def kernel(cfg, lens, hid, tabs, gain, bias, wq, wk, wv, wo, wu, wd,
           hbuf, kc, vc,
           wbuf, kraw, vraw, wkv, kvs, acc, abuf, pbuf, rbuf, xrecv, xres,
           wsem, ksem, vsem, iosem,
           d_send, d_recv, x_send, x_recv,
           gx_send, gx_recv, gc_send, gc_recv, gf_send, gf_recv):
    layers, seq, d, heads, scale = cfg
    nch = d // CH
    qw = heads * 128
    nq = qw // CH
    half = seq // 2
    part = half // 4
    kper = nch // nq
    both = slice(None)
    spare = heads + 4

    me = lax.axis_index("tp")
    mx = me // 2
    mc = me % 2
    core_peer = {"tp": mx * 2 + (1 - mc)}
    chip_peer = {"tp": (1 - mx) * 2 + mc}
    own = 2 * mc + mx
    peer = 2 * mc + 1 - mx
    away = pl.ds(2 * (1 - mc), 2)
    length = lens[0]

    def cols(j):
        if isinstance(j, int):
            return pl.ds(j * CH, CH)
        return pl.ds(pl.multiple_of(j * CH, CH), CH)

    def loop(n, body):
        lax.fori_loop(0, n, lambda i, c: (body(i), c)[1], 0)

    def sem(hf, j):
        return j if hf is both else hf * nch + j

    def span(hf, j):
        width = CH if hf is both else 2 * CH
        return pl.ds(j * width if isinstance(j, int) else pl.multiple_of(j * width, width), width)

    def spans(hf):
        return nch if hf is both else nch // 2

    def fetch_q(l, i, slot):
        rows = kper * CH
        for n in range(nq):
            for hh in range(4):
                pltpu.make_async_copy(
                    wq.at[l, 4 * n + hh, pl.ds(pl.multiple_of(i * rows, rows), rows), :],
                    wbuf.at[slot, pl.ds(n * rows, rows), pl.ds(hh * 128, 128)],
                    wsem.at[slot]).start()

    def fetch_o(l, i, slot):
        for n in range(kper):
            pltpu.make_async_copy(
                wo.at[l, :, cols(i * kper + n)],
                wbuf.at[slot, pl.ds(n * qw, qw), :],
                wsem.at[slot]).start()

    def fetch_u(l, i, slot):
        for n in range(nch):
            pltpu.make_async_copy(
                wu.at[l, cols(i), pl.ds(n * CH, CH)],
                wbuf.at[slot, pl.ds(n * CH, CH), :],
                wsem.at[slot]).start()

    def fetch_d(l, i, slot):
        pltpu.make_async_copy(wd.at[l, :, cols(i)], wbuf.at[slot], wsem.at[slot]).start()

    def weights_ready(slot):
        pltpu.make_async_copy(wd.at[0, :, pl.ds(0, CH)], wbuf.at[slot], wsem.at[slot]).wait()

    def kv_copies(l, kk):
        slot = kk % KV_RING
        rows = cols(kk)
        return (pltpu.make_async_copy(wk.at[l, rows, me], kraw.at[slot], ksem.at[slot]),
                pltpu.make_async_copy(wv.at[l, rows, me], vraw.at[slot], vsem.at[slot]))

    def kv_fetch(l, kk):
        for c in kv_copies(l, kk):
            c.start()

    def unpack(l, kk):
        for c in kv_copies(l, kk):
            c.wait()
        ks = kk % KV_RING

        size = 2 * part

        def piece(b):
            rows = pl.ds(pl.multiple_of(b * size, size), size)
            out = pl.ds(pl.multiple_of(kk * CH + b * size, size), size)
            for m, raw in enumerate((kraw, vraw)):
                acc[spare + m, pl.ds(0, 2 * size), :] = raw[ks, rows].astype(F32).reshape(2 * size, 128)
            for m in range(2):
                for n in range(2):
                    wkv[out, pl.ds((2 * m + n) * 128, 128)] = (
                        acc[spare + m, pl.ds(n, size, stride=2), :].astype(BF16))

        loop(CH // size, piece)

        @pl.when(kk + KV_RING < nch)
        def _():
            kv_fetch(l, kk + KV_RING)
        if l + 1 < layers:
            @pl.when(kk + KV_RING >= nch)
            def _():
                kv_fetch(l + 1, kk + KV_RING - nch)

    def remote(src, dst, ssem, rsem, peer_id):
        return pltpu.make_async_remote_copy(
            src_ref=src, dst_ref=dst, send_sem=ssem, recv_sem=rsem,
            device_id=peer_id, device_id_type=MESH)

    def d_copy(hf, j):
        i = sem(hf, j)
        return remote(pbuf.at[hf, away, :, span(hf, j)], rbuf.at[hf, :, :, span(hf, j)],
                      d_send.at[i], d_recv.at[i], core_peer)

    def x_copy(hf, j):
        i = sem(hf, j)
        return remote(pbuf.at[hf, peer, :, span(hf, j)], xrecv.at[hf, :, span(hf, j)],
                      x_send.at[i], x_recv.at[i], chip_peer)

    def rs_mid(hf, j):
        d_copy(hf, j).wait_recv()
        s = pbuf[hf, peer, :, span(hf, j)].astype(F32) + rbuf[hf, 1 - mx, :, span(hf, j)].astype(F32)
        pbuf[hf, peer, :, span(hf, j)] = s.astype(BF16)
        x_copy(hf, j).start()

    def rs_fin(hf, j):
        x_copy(hf, j).wait_recv()
        s = pbuf[hf, own, :, span(hf, j)].astype(F32) + rbuf[hf, mx, :, span(hf, j)].astype(F32)
        s = (s + xrecv[hf, :, span(hf, j)].astype(F32)).astype(BF16)
        new = (xres[hf, :, span(hf, j)].astype(F32) + s.astype(F32)).astype(BF16)
        xres[hf, :, span(hf, j)] = new
        return new

    def rs_fin_all(hf):
        loop(spans(hf), lambda j: (rs_fin(hf, j), None)[1])

    def rs_drain(hf):
        def body(j):
            d_copy(hf, j).wait_send()
            x_copy(hf, j).wait_send()
        loop(spans(hf), body)

    def gx_copy(hf, j):
        r, i = hbuf.at[hf, own, :, span(hf, j)], sem(hf, j)
        return remote(r, r, gx_send.at[i], gx_recv.at[i], chip_peer)

    def gc_copy(hf, j):
        r, i = hbuf.at[hf, own, :, span(hf, j)], sem(hf, j)
        return remote(r, r, gc_send.at[i], gc_recv.at[i], core_peer)

    def gf_copy(hf, j):
        r, i = hbuf.at[hf, peer, :, span(hf, j)], sem(hf, j)
        return remote(r, r, gf_send.at[i], gf_recv.at[i], core_peer)

    def gather_send(hf, j):
        gx_copy(hf, j).start()
        gc_copy(hf, j).start()

    def forward(hf, j):
        gx_copy(hf, j).wait_recv()
        gf_copy(hf, j).start()

    def gathered(hf, j):
        gc_copy(hf, j).wait_recv()
        gf_copy(hf, j).wait_recv()

    def gather_sent(hf):
        def body(j):
            gx_copy(hf, j).wait_send()
            gc_copy(hf, j).wait_send()
            gf_copy(hf, j).wait_send()
        loop(spans(hf), body)

    def norm(rows, load, layer, which, store):
        def fold(x):
            return sum(x[:, k * 128:(k + 1) * 128] for k in range(CH // 128))

        zero = jnp.zeros((rows, 128), F32)
        total = lax.fori_loop(0, nch, lambda j, t: t + fold(load(j)), zero)
        mean = jnp.sum(total, axis=-1, keepdims=True) * (1.0 / d)

        def squares(j, t):
            x = load(j) - mean
            return t + fold(x * x)

        var = jnp.sum(lax.fori_loop(0, nch, squares, zero), axis=-1, keepdims=True) * (1.0 / d)
        rstd = lax.rsqrt(var + NORM_EPS)

        def write(j):
            x = (load(j) - mean) * rstd
            g = gain[layer, pl.ds(which, 1), cols(j)]
            b = bias[layer, pl.ds(which, 1), cols(j)]
            store(j, (x * (1.0 + g) + b).astype(BF16))

        loop(nch, write)

    def norm_own(hf, layer, which, sent):
        def store(j, y):
            hbuf[hf, own, :, cols(j)] = y

            @pl.when((j % 2 == 1) & (j < 2 * sent))
            def _():
                gather_send(hf, j // 2)

        norm(part, lambda j: xres[hf, :, cols(j)].astype(F32), layer, which, store)

    def clear(first, count, blocks):
        def body(i):
            acc[i, pl.ds(first, count), :] = jnp.zeros((count, 128), F32)
        loop(blocks, body)

    def add(n, first, count, value):
        for t in range(CH // 128):
            acc[n * (CH // 128) + t, pl.ds(first, count), :] += value[:, t * 128:(t + 1) * 128]

    def project(l, hf):
        rows, count = (0, seq) if hf is both else (hf * half, half)
        clear(rows, count, spare)
        if l > 0:
            forward(hf, 0)

        def group(i):
            if hf is both or hf == 0:
                weights_ready(i)

            def chunk(kq):
                kk = i * kper + kq
                if l > 0:
                    if hf == 0:
                        unpack(l, kk)

                    @pl.when((kk % 2 == 0) & (kk + 2 < nch))
                    def _():
                        forward(hf, kk // 2 + 1)

                    @pl.when(kk % 2 == 0)
                    def _():
                        gathered(hf, kk // 2)
                hk = hbuf[hf, :, :, cols(kk)].reshape(count, CH)
                for n in range(nq):
                    w = wbuf[i, pl.ds(pl.multiple_of(n * kper * CH + kq * CH, CH), CH), :]
                    add(n, rows, count, jnp.dot(hk, w, preferred_element_type=F32))
                add(nq, rows, count, jnp.dot(hk, wkv[cols(kk), :], preferred_element_type=F32))

            loop(kper, chunk)
            if hf is both or hf == 1:
                fetch_u(l, i, i)

        loop(nq, group)

    def attention(l, hf):
        cosine, sin_a, sin_b = (tabs[t, pl.ds(hf * half, half), :] for t in range(3))
        rows, width = pl.ds(hf * half, half), seq
        row = lax.broadcasted_iota(jnp.int32, (half, 128), 0) + hf * half
        live = row < length

        def rope(x):
            return x * cosine + pltpu.roll(x, 96, 1) * sin_a + pltpu.roll(x, 32, 1) * sin_b

        for n in range(2):
            k = rope(acc[heads + n, rows, :])
            v = acc[heads + 2 + n, rows, :]
            kvs[rows, pl.ds(n * 128, 128)] = k.astype(BF16)
            kvs[rows, pl.ds((n + 2) * 128, 128)] = v.astype(BF16)
            acc[spare, pl.ds(n, half, stride=2), :] = jnp.where(live, k, 0.0)
            acc[spare + 1, pl.ds(n, half, stride=2), :] = jnp.where(live, v, 0.0)
        kc[l, 0, rows] = acc[spare].reshape(half, 2, 128).astype(BF16)
        vc[l, 0, rows] = acc[spare + 1].reshape(half, 2, 128).astype(BF16)

        group = heads // 2
        limit = jnp.minimum(lax.broadcasted_iota(jnp.int32, (half, width), 0) + hf * half, length - 1)
        allowed = lax.broadcasted_iota(jnp.int32, (half, width), 1) <= limit
        pace = scale * 1.4426950408889634

        def body(i):
            for n in range(2):
                k = kvs[:, pl.ds(n * 128, 128)]
                v = kvs[:, pl.ds((n + 2) * 128, 128)]
                for t in range(2):
                    j = n * group + 2 * i + t
                    lanes = pl.ds(pl.multiple_of(j * 128, 128), 128)
                    q = rope(acc[j, rows, :]).astype(BF16)
                    s = lax.dot_general(q, k, (((1,), (1,)), ((), ())), preferred_element_type=F32)
                    s = jnp.where(allowed, s, -1e30)
                    e = jnp.exp2((s - jnp.max(s, axis=-1, keepdims=True)) * pace)
                    p = (e * (1.0 / jnp.sum(e, axis=-1, keepdims=True))).astype(BF16)
                    abuf[rows, lanes] = jnp.dot(p, v, preferred_element_type=F32).astype(BF16)

        loop(group // 2, body)

    def project_out(l, hf):
        rows = pl.ds(hf * half, half)

        def group(i):
            slot = nq + i
            if hf == 0:
                weights_ready(slot)

            def pair(n):
                j = i * (kper // 2) + n
                for t in range(2):
                    w = wbuf[slot, pl.ds(pl.multiple_of((2 * n + t) * qw, qw), qw), :]
                    o = jnp.dot(abuf[rows, pl.ds(0, qw)], w, preferred_element_type=F32)
                    pbuf[hf, :, :, cols(2 * j + t)] = o.astype(BF16).reshape(4, part, CH)
                d_copy(hf, j).start()

                @pl.when(j >= LAG)
                def _():
                    rs_mid(hf, j - LAG)

            loop(kper // 2, pair)
            if hf == 1:
                fetch_u(l, slot, slot)

        loop(nq, group)

    def mlp_up(l):
        clear(0, seq, d // 128)
        forward(0, 0)
        forward(1, 0)

        def group(i):
            slot = i % RING

            @pl.when((i % 2 == 0) & (i + 2 < nch))
            def _():
                forward(0, i // 2 + 1)
                forward(1, i // 2 + 1)

            @pl.when(i % 2 == 0)
            def _():
                gathered(0, i // 2)
                gathered(1, i // 2)
            weights_ready(slot)
            hk = hbuf[:, :, :, cols(i)].reshape(seq, CH)
            for n in range(nch):
                add(n, 0, seq, jnp.dot(hk, wbuf[slot, pl.ds(n * CH, CH), :], preferred_element_type=F32))

            @pl.when(i < nch - RING)
            def _():
                fetch_u(l, i + RING, slot)

            @pl.when(i >= nch - RING)
            def _():
                fetch_d(l, i + RING - nch, slot)

        loop(nch, group)
        gather_sent(0)
        gather_sent(1)

        def square(j):
            for t in range(4):
                u = jnp.maximum(acc[4 * j + t], 0.0)
                abuf[:, pl.ds(pl.multiple_of(j * CH + t * 128, 128), 128)] = (u * u).astype(BF16)

        loop(nch, square)

    def finish(j):
        hbuf[:, own, :, cols(j)] = rs_fin(both, j)
        gather_send(both, j)

    def mlp_down(l):
        last = l + 1 == layers

        def group(j):
            slot = j % RING
            weights_ready(slot)
            m = jnp.dot(abuf[...], wbuf[slot], preferred_element_type=F32)
            pbuf[:, :, :, cols(j)] = m.astype(BF16).reshape(2, 4, part, CH)
            d_copy(both, j).start()

            @pl.when(j < nch - RING)
            def _():
                fetch_d(l, j + RING, slot)
            if not last:
                @pl.when((j >= nch - RING) & (j < nch - RING + nq))
                def _():
                    fetch_q(l + 1, j - (nch - RING), slot)

                @pl.when(j >= nch - RING + nq)
                def _():
                    fetch_o(l + 1, j - (nch - RING + nq), slot)

            @pl.when(j >= 1)
            def _():
                rs_mid(both, j - 1)
            if last:
                @pl.when(j >= 3)
                def _():
                    finish(j - 3)

                @pl.when(j >= 5)
                def _():
                    forward(both, j - 5)

        loop(nch, group)
        rs_mid(both, nch - 1)
        if not last:
            rs_fin_all(both)
        else:
            for j in range(nch - 3, nch):
                finish(j)
            for j in range(nch - 5, nch):
                forward(both, j)
            loop(nch, lambda j: gathered(both, j))
        rs_drain(both)

    load = pltpu.make_async_copy(hid, pbuf, iosem.at[0])
    load.start()
    for kk in range(KV_RING):
        kv_fetch(0, kk)
    barrier = pltpu.get_barrier_semaphore()
    for other in (core_peer, chip_peer):
        pl.semaphore_signal(barrier, inc=1, device_id=other, device_id_type=MESH)
    load.wait()

    for i in range(nq):
        fetch_q(0, i, i)
    xres[...] = pbuf[:, own]
    kvs[pl.ds(half, half), :] = jnp.zeros((half, CH), BF16)

    def first_norm(b):
        hf, o = b // 2, pl.ds(b % 2 * 2, 2)

        def store(j, y):
            hbuf[hf, o, :, cols(j)] = y.reshape(2, part, CH)

        norm(2 * part, lambda j: pbuf[hf, o, :, cols(j)].reshape(2 * part, CH).astype(F32), 0, 0, store)

    loop(4, first_norm)
    loop(nch, lambda kk: unpack(0, kk))
    for i in range(nq):
        fetch_o(0, i, nq + i)
    pl.semaphore_wait(barrier, 2)

    for l in range(layers):
        project(l, 0 if l > 0 else both)
        if l > 0:
            gather_sent(0)
        attention(l, 0)
        project_out(l, 0)
        loop(LAG, lambda j: rs_mid(0, spans(0) - LAG + j))
        if l > 0:
            project(l, 1)
            gather_sent(1)
        attention(l, 1)
        project_out(l, 1)
        loop(LAG, lambda j: rs_mid(1, spans(1) - LAG + j))
        rs_fin_all(0)
        norm_own(0, l, 1, EARLY)
        rs_fin_all(1)
        norm_own(1, l, 1, EARLY)

        def rest(j):
            gather_send(0, EARLY + j)
            gather_send(1, EARLY + j)

        loop(spans(0) - EARLY, rest)
        rs_drain(0)
        rs_drain(1)
        mlp_up(l)
        mlp_down(l)
        if l + 1 < layers:
            norm_own(0, l + 1, 0, spans(0))
            norm_own(1, l + 1, 0, spans(1))

    gather_sent(both)


def solution(mesh):
    def device_body(hidden_in, lengths, positions, ln_gain, ln_bias, w_query, w_key, w_value, w_out, w_up, w_down):
        seq, d = hidden_in.shape[1], hidden_in.shape[2]
        layers, _, heads, head = w_query.shape
        kv_heads = w_key.shape[2]
        tp = mesh.shape["tp"]
        kv = kv_heads // tp
        nch = d // CH

        half_rot = head // 4
        lane = jnp.arange(head)
        freq = ROPE_BASE ** (-2.0 * (lane % half_rot).astype(F32) / (2 * half_rot))
        angle = positions[0].astype(F32)[:, None] * freq
        cos, sin = jnp.cos(angle), jnp.sin(angle)
        tabs = jnp.stack([
            jnp.where(lane < 2 * half_rot, cos, 1.0),
            jnp.where(lane < half_rot, -sin, 0.0),
            jnp.where((lane >= half_rot) & (lane < 2 * half_rot), sin, 0.0)])

        vmem = pl.BlockSpec(memory_space=pltpu.VMEM)
        smem = pl.BlockSpec(memory_space=pltpu.SMEM)
        anym = pl.BlockSpec(memory_space=pl.ANY)
        dma = pltpu.SemaphoreType.DMA
        cfg = (layers, seq, d, heads, head ** -0.5)
        rows = (2, 4, seq // 8)
        out, kc, vc = pl.pallas_call(
            functools.partial(kernel, cfg),
            out_shape=(pltpu.VMEM(rows + (d,), BF16),
                       pltpu.VMEM((layers, 1, seq, kv, head), BF16),
                       pltpu.VMEM((layers, 1, seq, kv, head), BF16)),
            in_specs=[smem, anym, vmem, vmem, vmem] + [anym] * 6,
            out_specs=(vmem, vmem, vmem),
            scratch_shapes=[
                pltpu.VMEM((RING, d, CH), BF16),
                pltpu.VMEM((KV_RING, CH, kv, head), BF16),
                pltpu.VMEM((KV_RING, CH, kv, head), BF16),
                pltpu.VMEM((d, 2 * kv * head), BF16),
                pltpu.VMEM((seq, 2 * kv * head), BF16),
                pltpu.VMEM((d // head, seq, head), F32),
                pltpu.VMEM((seq, d), BF16),
                pltpu.VMEM(rows + (d,), BF16),
                pltpu.VMEM((2, 2, seq // 8, d), BF16),
                pltpu.VMEM((2, seq // 8, d), BF16),
                pltpu.VMEM((2, seq // 8, d), BF16),
                dma((RING,)), dma((KV_RING,)), dma((KV_RING,)), dma((2,)),
            ] + [dma((2 * nch,))] * 10,
            compiler_params=pltpu.CompilerParams(
                collective_id=0, has_side_effects=True, vmem_limit_bytes=VMEM_LIMIT),
            name="decoder_layers",
        )(lengths, hidden_in.reshape(rows + (d,)), tabs, ln_gain, ln_bias,
          w_query.transpose(0, 2, 1, 3),
          w_key.reshape(layers, d, tp, kv, head), w_value.reshape(layers, d, tp, kv, head),
          w_out.reshape(layers, heads * head, d), w_up, w_down)
        return out.reshape(1, seq, d), kc, vc

    specs_in = (P("dp", None, None), P("dp"), P("dp", None), P(), P(), P(None, None, "tp", None), P(), P(),
                P(None, "tp", None, None), P(None, None, "tp"), P(None, "tp", None))
    cache_spec = P(None, "dp", None, "tp", None)
    return jax.shard_map(device_body, mesh=mesh, in_specs=specs_in,
                         out_specs=(P("dp", None, None), cache_spec, cache_spec), check_vma=False)
```
